256 devices in a mesh: rep: 4 (over z_hi, core), dom: 64 (over z_lo, y, x).
Axes of the slice: x: 4, y: 4, z: 8 (z_hi: 2, z_lo: 4; z = z_hi * 4 + z_lo), core: 2. Of those that a mesh axis runs over, the one named last changes fastest.
Arguments:
- positions: float32 [3, 2097152], P(None, ('rep', 'dom')), parts along dimension 1, may hold values from -4 to 4
- velocities: float32 [3, 2097152], P(None, ('rep', 'dom')), parts along dimension 1, may hold values from -5 to 5
- charges: float32 [2097152], P(('rep', 'dom')), parts along dimension 0, may hold values from -4 to 4
- solute: int32 [2097152], P(('rep', 'dom')), parts along dimension 0, may hold values 0 or 1
- rest_scale: float32 [4], P('rep'), parts along dimension 0, may hold values from 0.25 to 1
- send_slot: int32 [256, 64], P(('rep', 'dom')), parts along dimension 0, may hold values from 0 to 64, as said below
- land_slot: int32 [256, 64], P(('rep', 'dom')), parts along dimension 0, may hold values from 0 to 64, as said below
- ghost_slot: int32 [256, 64], P(('rep', 'dom')), parts along dimension 0, may hold values from 0 to 63
- pair_home: int32 [256, 192], P(('rep', 'dom')), parts along dimension 0, may hold values from 0 to 63
- pair_other: int32 [256, 192], P(('rep', 'dom')), parts along dimension 0, may hold values from 0 to 127, as said below
Outputs:
- positions_out: float32 [3, 2097152], P(None, ('rep', 'dom')), parts along dimension 1
- velocities_out: float32 [3, 2097152], P(None, ('rep', 'dom')), parts along dimension 1
- forces_out: float32 [3, 2097152], P(None, ('rep', 'dom')), parts along dimension 1
The draws below stay inside these ranges and needn't reach their ends.
There are 4 independent parts, one for each index of `rep`. The reference program is written for one: setup_inputs(seed, part) draws one part's arguments, and reference() takes and returns one part's arrays. A program takes and returns all parts, laid end to end along the dimension named above; each array names one. Nothing has to cross between parts.
Inputs may be any that keep to these rules, and one draw needn't show every extreme that they name: `send_slot`: entry [d, p] is the slot of the block domain d hands to domain p, or 64 where it hands none; each domain hands 32 distinct blocks to 32 distinct other domains, and each domain receives from 32 domains. `land_slot`: entry [d, p] is the slot that the block arriving at d from p takes, or 64 exactly where send_slot[p, d] is 64; the slots a domain fills are exactly the slots it hands over. `pair_other`: in every row the first 128 entries are below 64; the other 64 are 64 or more, and every ghost slot appears among them at least once.
All inputs are finite; a program needn't handle non-finite values. No bound on the sum of `solute` on one device may be relied on, other than what follows from the above.
Results may differ from the reference program's by a relative error of at most 0.0001.
Values sent between devices are 32-bit elements; how exact they have to be, the bound alone decides.
No kernel may reach another device: no remote copies, remote signals or barrier semaphores. Data moves between devices by JAX's collectives and lax.ppermute only.
A program may use at most 64 MiB of HBM per device.

```python
import math
import jax
import jax.numpy as jnp
from jax import lax

BLOCK = 128
B_DEV = 64
STEPS = 2
MOVE = 32
GHOST_DEV = 64
GCAP = 1
LPAIRS = 128
GPAIRS = 64
PAIRS = 192
ATOMS = 524288
N_DOM = 64


def migration_plan(key):
    base = jax.random.fold_in(key, 17)
    first_key, second_key, third_key = jax.random.split(base, 3)
    offsets = 1 + jax.random.permutation(first_key, N_DOM - 1)[:MOVE]
    order_map = jax.random.permutation(second_key, N_DOM)
    inverse = jnp.argsort(order_map, stable=True)
    slots = jax.vmap(lambda subkey: jax.random.permutation(subkey, B_DEV)[:MOVE])(jax.random.split(third_key, N_DOM))
    domains = jnp.arange(N_DOM, dtype=jnp.int32)
    position = inverse[domains][:, None]
    destination = order_map[(position + offsets[None, :]) % N_DOM]
    anchor = order_map[(position - offsets[None, :]) % N_DOM]
    vacant = jnp.full((N_DOM, N_DOM), B_DEV, jnp.int32)
    handed = vacant.at[domains[:, None], destination].set(slots.astype(jnp.int32))
    landing = vacant.at[domains[:, None], anchor].set(slots.astype(jnp.int32))
    return (handed, landing)


def draw_send_slot(key, part):
    return migration_plan(key)[0]


def draw_land_slot(key, part):
    return migration_plan(key)[1]


def draw_pair_other(key, part):
    base = jax.random.fold_in(key, 29)
    first_key, second_key, third_key = jax.random.split(base, 3)
    nearby = jax.random.randint(first_key, (N_DOM, LPAIRS), 0, B_DEV)
    extra = jax.random.randint(second_key, (N_DOM, GPAIRS - GHOST_DEV), 0, GHOST_DEV)
    covered = jnp.broadcast_to(jnp.arange(GHOST_DEV, dtype=jnp.int32), (N_DOM, GHOST_DEV))
    chosen = jnp.concatenate([covered, extra.astype(jnp.int32)], 1)
    shuffled = jax.vmap(lambda subkey, entries: jax.random.permutation(subkey, entries))(jax.random.split(third_key, N_DOM), chosen)
    return jnp.concatenate([nearby.astype(jnp.int32), B_DEV + shuffled], 1).astype(jnp.int32)


def with_ends(values, stream_key, least, top_value):
    longest = values.shape.index(max(values.shape))
    spots = []
    for shift in (0, 1):
        where = [jax.random.randint(jax.random.fold_in(stream_key, axis), (), 0, length) for axis, length in enumerate(values.shape)]
        where[longest] = (where[longest] + shift) % values.shape[longest]
        spots.append(tuple(where))
    return values.at[spots[0]].set(least).at[spots[1]].set(top_value)


def block_levels(rng, extent, cuts, smallest, largest):
    gain = 1.0
    for dim, shards_of in cuts:
        heights = jax.random.uniform(jax.random.fold_in(jax.random.fold_in(rng, 6), dim), (shards_of,), jnp.float32, smallest / len(cuts), largest / len(cuts))
        gain = gain * jnp.repeat(jnp.exp(heights), extent[dim] // shards_of).reshape((-1,) + (1,) * (len(extent) - 1 - dim))
    return gain


def scatter_about(stream_key, shape, spread, limit, cuts=(), kind=jnp.bfloat16):
    drawn = jax.random.normal(stream_key, shape, jnp.float32) * spread
    if len(cuts) > 0:
        drawn = block_levels(stream_key, shape, cuts, -0.22, 0.18) * drawn
    return jnp.clip(drawn, min=-limit, max=limit).astype(kind)


def setup_inputs(seed: int = 0, part: int = 0) -> dict:
    key_of = jax.random.split(jax.random.key(seed), 11)
    part_keys = jax.random.split(jax.random.fold_in(key_of[10], part), 11)
    return {
        "positions": scatter_about(part_keys[0], (3, ATOMS), 1.0, 4.0, ((1, 64),), jnp.float32),
        "velocities": scatter_about(part_keys[1], (3, ATOMS), 1.0, 5.0, ((1, 64),), jnp.float32),
        "charges": scatter_about(part_keys[2], (ATOMS,), 1.0, 4.0, ((0, 64),), jnp.float32),
        "solute": with_ends((jax.random.randint(part_keys[3], (ATOMS,), 0, 5) < 2).astype(jnp.int32), jax.random.fold_in(part_keys[3], 1), 0, 1),
        "rest_scale": jnp.clip(jnp.exp(jax.random.uniform(part_keys[4], (1,), jnp.float32, math.log(0.25), math.log(1.0))), 0.25, 1.0),
        "send_slot": draw_send_slot(jax.random.fold_in(jax.random.fold_in(key_of[10], part), 71), part),
        "land_slot": draw_land_slot(jax.random.fold_in(jax.random.fold_in(key_of[10], part), 71), part),
        "ghost_slot": with_ends(jax.random.randint(part_keys[7], (N_DOM, GHOST_DEV), 0, B_DEV), jax.random.fold_in(part_keys[7], 1), 0, B_DEV - 1).astype(jnp.int32),
        "pair_home": with_ends(jax.random.randint(part_keys[8], (N_DOM, PAIRS), 0, B_DEV), jax.random.fold_in(part_keys[8], 1), 0, B_DEV - 1).astype(jnp.int32),
        "pair_other": draw_pair_other(jax.random.fold_in(jax.random.fold_in(key_of[10], part), 71), part),
    }


coupling_scale = 0.2
time_step = 0.05
highest = lax.Precision.HIGHEST

def tile_forces(left_coords, left_params, right_coords, right_params):
    inner = lax.dot_general(left_coords, right_coords, (((0,), (0,)), ((), ())), precision=highest, preferred_element_type=jnp.float32)
    squared = lax.optimization_barrier(jnp.sum(left_coords * left_coords, 0))[:, None] + lax.optimization_barrier(jnp.sum(right_coords * right_coords, 0))[None, :] - 2.0 * inner
    decay = jnp.exp(-0.5 * squared)
    coupling = coupling_scale * (left_params[0][:, None] * right_params[0][None, :] * decay + left_params[1][:, None] * right_params[1][None, :] * decay * decay)
    left_force = left_coords * lax.optimization_barrier(jnp.sum(coupling, 1))[None, :] - lax.dot_general(right_coords, coupling, (((1,), (1,)), ((), ())), precision=highest, preferred_element_type=jnp.float32)
    right_force = right_coords * lax.optimization_barrier(jnp.sum(coupling, 0))[None, :] - jnp.dot(left_coords, coupling, precision=highest, preferred_element_type=jnp.float32)
    return (left_force, right_force)

def all_forces(coords, params, home_ids, other_ids):

    def one_group(indices):
        home_rows, other_rows = indices
        return jax.vmap(tile_forces)(coords[home_rows], params[home_rows], coords[other_rows], params[other_rows])
    shaped = (home_ids.reshape(-1, 64), other_ids.reshape(-1, 64))
    home_force, other_force = lax.map(one_group, shaped)
    totals = jnp.zeros_like(coords)
    totals = totals.at[home_ids].add(home_force.reshape((-1,) + coords.shape[1:]))
    return totals.at[other_ids].add(other_force.reshape((-1,) + coords.shape[1:]))

def reference(positions, velocities, charges, solute, rest_scale, send_slot, land_slot, ghost_slot, pair_home, pair_other):
    weight = jnp.where(solute == 1, jnp.sqrt(rest_scale[0]), 1.0).astype(jnp.float32)
    params = jnp.stack([weight * charges, weight])
    states = jnp.concatenate([positions, velocities, params], 0)
    states = states.reshape(8, N_DOM * B_DEV, BLOCK).transpose(1, 0, 2).reshape(N_DOM, B_DEV, 8, BLOCK)
    domains = jnp.arange(N_DOM, dtype=jnp.int32)
    padded = jnp.concatenate([states, jnp.zeros((N_DOM, 1, 8, BLOCK), states.dtype)], 1)
    incoming = send_slot.T
    moved = padded[domains[None, :], incoming]
    placed = padded.at[domains[:, None], land_slot].set(moved)[:, :B_DEV]
    placed = placed.reshape(N_DOM * B_DEV, 8, BLOCK)
    ghost_index = jnp.maximum(pair_other - B_DEV, 0)
    source = (ghost_index // GCAP).astype(jnp.int32)
    within = (ghost_index % GCAP).astype(jnp.int32)
    remote = ghost_slot[source, domains[:, None] * GCAP + within]
    other_ids = jnp.where(pair_other < B_DEV, domains[:, None] * B_DEV + pair_other, source * B_DEV + remote).astype(jnp.int32).reshape(-1)
    home_ids = (domains[:, None] * B_DEV + pair_home).astype(jnp.int32).reshape(-1)
    coords = placed[:, :3]
    speeds = placed[:, 3:6]
    params_now = placed[:, 6:]
    forces = jnp.zeros_like(coords)
    for step_index in range(STEPS):
        forces = all_forces(coords, params_now, home_ids, other_ids)
        speeds = speeds + time_step * forces
        coords = coords + time_step * speeds

    def flatten(values):
        return values.transpose(1, 0, 2).reshape(3, N_DOM * B_DEV * BLOCK)
    return (flatten(coords), flatten(speeds), flatten(forces))
```

```python
import math

import jax
import jax.numpy as jnp
from jax import lax
from jax.experimental import pallas as pl
from jax.experimental.pallas import tpu as pltpu
from jax.sharding import PartitionSpec as P

BLOCK = 128
BLOCKS = 64
DOMAINS = 64
LOCAL = 128
GHOST = 64

coupling_scale = 0.2
time_step = 0.05
root_log2e = math.sqrt(math.log2(math.e))
local_unroll = 32
ghost_unroll = 16
f32 = jnp.float32
bf16 = jnp.bfloat16

vmem = pl.BlockSpec(memory_space=pltpu.VMEM)
smem = pl.BlockSpec(memory_space=pltpu.SMEM)


def rounded(values):
    return values.astype(bf16).astype(f32)


def split3(values):
    first = rounded(values)
    rest = values - first
    second = rounded(rest)
    return first, second, rounded(rest - second)


def exponent_parts(coords):
    scaled = coords * root_log2e
    half = 0.5 * jnp.sum(scaled * scaled, 0, keepdims=True)
    return split3(jnp.concatenate([scaled, half, scaled, half], 0))


def row_masks():
    row = lax.broadcasted_iota(jnp.int32, (8, BLOCK), 0)
    return row == 3, row == 7, row < 4


def source_rows(parts, charge):
    p0, p1, p2 = parts
    third, last, low = row_masks()
    s0 = jnp.where(third, -p0, jnp.where(last, -p1, p0))
    s1 = jnp.where(third, -p2, jnp.where(last, 1.0, p1))
    s2 = jnp.where(third | last, 1.0, jnp.where(low, p0, p2))
    return jnp.concatenate([s0, s1, s2, jnp.broadcast_to(charge, (8, BLOCK))], 0)


def target_rows(parts):
    p0, p1, p2 = parts
    third, last, low = row_masks()
    t0 = jnp.where(third | last, 1.0, jnp.where(low, p0, p1))
    t1 = jnp.where(third, 1.0, jnp.where(last, -p0, jnp.where(low, p0, p1)))
    t2 = jnp.where(third, -p1, jnp.where(last, -p2, jnp.where(low, p2, p0)))
    return jnp.concatenate([t0, t1, t2, jnp.zeros((8, BLOCK), f32)], 0).astype(bf16)


def weight_rows(coords, weight):
    low = row_masks()[2]
    ones = jnp.ones((1, BLOCK), f32)
    w0, w1, w2 = split3(jnp.concatenate([coords, ones, coords, ones], 0) * weight)
    return jnp.concatenate([jnp.where(low, w0, w1), jnp.where(low, w2, 0.0)], 0).astype(bf16)


def coupled_sums(sources, charges, weights, targets, target_charges):
    empty = jnp.zeros((32, BLOCK), bf16)
    right = jnp.concatenate(
        [
            jnp.concatenate([targets[0], empty], 1),
            jnp.concatenate([empty, targets[1]], 1),
        ],
        0,
    )
    exponent = jnp.dot(sources, right, preferred_element_type=f32)
    tiles = []
    for which in range(2):
        decay = jnp.exp2(exponent[:, which * BLOCK : (which + 1) * BLOCK])
        tiles.append(decay * (charges[which] * target_charges[which] + decay))
    coupling = jnp.concatenate(tiles, 1)
    high = coupling.astype(bf16)
    low = (coupling - high.astype(f32)).astype(bf16)
    stacked = jnp.concatenate([high, low], 0)
    left = jnp.concatenate(weights, 0)
    left = jnp.concatenate([left, left], 1)
    return jnp.dot(left, stacked, preferred_element_type=f32)


def pack_kernel(scale, send, positions, velocities, charges, solute, states, outbound):
    root = jnp.sqrt(jnp.full((8, BLOCK), scale[0], f32))

    def gather(group, carry):
        first = pl.multiple_of(group * 8, 8)
        charge_rows = charges[pl.ds(first, 8), :]
        weight = jnp.where(solute[pl.ds(first, 8), :] == 1, root, 1.0)
        for inner in range(8):
            lanes = pl.ds(pl.multiple_of((group * 8 + inner) * BLOCK, BLOCK), BLOCK)
            states[group * 8 + inner] = jnp.concatenate(
                [
                    positions[:, lanes],
                    velocities[:, lanes],
                    charge_rows[inner : inner + 1],
                    weight[inner : inner + 1],
                ],
                0,
            )
        return carry

    lax.fori_loop(0, BLOCKS // 8, gather, 0)

    def hand_over(group, carry):
        for inner in range(8):
            peer = group * 8 + inner
            outbound[peer] = states[jnp.minimum(send[0, peer], BLOCKS - 1)]
        return carry

    lax.fori_loop(0, DOMAINS // 8, hand_over, 0)


def home_table(home, other, homes):
    def enter(entry, carry):
        homes[other[0, LOCAL + entry] - BLOCKS] = home[0, LOCAL + entry]
        return carry

    lax.fori_loop(0, GHOST, enter, 0)


def place_kernel(land, ghost, home, other, states, arrived, placed, outgoing, homes):
    home_table(home, other, homes)

    def keep(group, carry):
        placed[pl.ds(group * 8, 8)] = states[pl.ds(group * 8, 8)]
        return carry

    lax.fori_loop(0, BLOCKS // 8, keep, 0)

    def receive(group, carry):
        for inner in range(8):
            peer = group * 8 + inner
            placed[land[0, peer]] = arrived[peer]
        return carry

    lax.fori_loop(0, DOMAINS // 8, receive, 0)

    def send(group, carry):
        for inner in range(8):
            peer = group * 8 + inner
            for which, slot in enumerate((ghost[0, peer], homes[peer])):
                for column, row in enumerate((0, 1, 2, 6, 7)):
                    outgoing[peer, which : which + 1, column * BLOCK : (column + 1) * BLOCK] = (
                        placed[slot, row : row + 1, :]
                    )
        return carry

    lax.fori_loop(0, DOMAINS // 8, send, 0)


def local_kernel(home, other, placed, sums, targets, first, second, weights, spread):
    def prepare(group, carry):
        stacked = []
        for inner in range(4):
            block = group * 4 + inner
            state = placed[block]
            parts = exponent_parts(state[0:3])
            targets[block] = target_rows(parts)
            weights[block] = weight_rows(state[0:3], state[7:8])
            stacked.append(source_rows(parts, state[6:7]))
            sums[block] = jnp.zeros((16, BLOCK), f32)
        columns = jnp.concatenate(stacked, 0).T
        empty = jnp.zeros((BLOCK, 32), bf16)
        for inner in range(4):
            block = group * 4 + inner
            chosen = columns[:, inner * 32 : (inner + 1) * 32]
            narrow = chosen.astype(bf16)
            first[block] = jnp.concatenate([narrow, empty], 1)
            second[block] = jnp.concatenate([empty, narrow], 1)
            spread[block] = jnp.broadcast_to(chosen[:, 24:25], (BLOCK, BLOCK))
        return carry

    lax.fori_loop(0, BLOCKS // 4, prepare, 0)

    def pairs(group, carry):
        for inner in range(local_unroll):
            entry = group * local_unroll + inner
            one = home[0, entry]
            two = other[0, entry]
            result = coupled_sums(
                first[two] + second[one],
                (spread[two], spread[one]),
                (weights[two], weights[one]),
                (targets[one], targets[two]),
                (placed[one, 6:7, :], placed[two, 6:7, :]),
            )
            sums[one] += result[:16, :BLOCK]
            sums[two] += result[16:, BLOCK:]
        return carry

    lax.fori_loop(0, LOCAL // local_unroll, pairs, 0)


def ghost_pairs(ghost, homes, placed, targets, sums, total, coords_of, params_of):
    def start(group, carry):
        total[pl.ds(group * 8, 8)] = sums[pl.ds(group * 8, 8)]
        return carry

    lax.fori_loop(0, BLOCKS // 8, start, 0)

    def pairs(group, carry):
        for half in range(ghost_unroll // 2):
            stacked = []
            weights = []
            for inner in range(2):
                peer = group * ghost_unroll + half * 2 + inner
                for which in range(2):
                    coords = coords_of(peer, which)
                    charge, weight = params_of(peer, which)
                    stacked.append(source_rows(exponent_parts(coords), charge))
                    weights.append(weight_rows(coords, weight))
            columns = jnp.concatenate(stacked, 0).T
            narrow = columns.astype(bf16)
            for inner in range(2):
                peer = group * ghost_unroll + half * 2 + inner
                one = homes[peer]
                two = ghost[0, peer]
                lane = inner * 64
                result = coupled_sums(
                    narrow[:, lane : lane + 64],
                    (
                        jnp.broadcast_to(columns[:, lane + 24 : lane + 25], (BLOCK, BLOCK)),
                        jnp.broadcast_to(columns[:, lane + 56 : lane + 57], (BLOCK, BLOCK)),
                    ),
                    (weights[inner * 2], weights[inner * 2 + 1]),
                    (targets[one], targets[two]),
                    (placed[one, 6:7, :], placed[two, 6:7, :]),
                )
                total[one] += result[:16, :BLOCK]
                total[two] += result[16:, BLOCK:]
        return carry

    lax.fori_loop(0, DOMAINS // ghost_unroll, pairs, 0)


def moved(state, total):
    folded = total[0:4] + total[4:8] + total[8:12]
    force = (coupling_scale * state[7:8]) * (state[0:3] * folded[3:4] - folded[0:3])
    speed = state[3:6] + time_step * force
    return state[0:3] + time_step * speed, speed, force


def middle_kernel(
    ghost, home, other, placed, sums, targets, received, updated, outgoing, homes, total
):
    home_table(home, other, homes)

    def row(peer, which, column):
        return received[peer, which : which + 1, column * BLOCK : (column + 1) * BLOCK]

    ghost_pairs(
        ghost,
        homes,
        placed,
        targets,
        sums,
        total,
        lambda peer, which: jnp.concatenate([row(peer, which, c) for c in range(3)], 0),
        lambda peer, which: (row(peer, which, 3), row(peer, which, 4)),
    )

    def step(group, carry):
        for inner in range(8):
            block = group * 8 + inner
            state = placed[block]
            coords, speed, _ = moved(state, total[block])
            updated[block] = jnp.concatenate([coords, speed, state[6:8]], 0)
        return carry

    lax.fori_loop(0, BLOCKS // 8, step, 0)

    def send(group, carry):
        for inner in range(8):
            peer = group * 8 + inner
            for which, slot in enumerate((ghost[0, peer], homes[peer])):
                for column in range(3):
                    outgoing[peer, which : which + 1, column * BLOCK : (column + 1) * BLOCK] = (
                        updated[slot, column : column + 1, :]
                    )
        return carry

    lax.fori_loop(0, DOMAINS // 8, send, 0)


def last_kernel(
    ghost,
    home,
    other,
    placed,
    sums,
    targets,
    received,
    earlier,
    coords_out,
    speeds_out,
    forces_out,
    homes,
    total,
):
    home_table(home, other, homes)

    def row(ref, peer, which, column):
        return ref[peer, which : which + 1, column * BLOCK : (column + 1) * BLOCK]

    ghost_pairs(
        ghost,
        homes,
        placed,
        targets,
        sums,
        total,
        lambda peer, which: jnp.concatenate([row(received, peer, which, c) for c in range(3)], 0),
        lambda peer, which: (row(earlier, peer, which, 3), row(earlier, peer, which, 4)),
    )

    def step(group, carry):
        for inner in range(8):
            block = group * 8 + inner
            coords, speed, force = moved(placed[block], total[block])
            lanes = pl.ds(pl.multiple_of(block * BLOCK, BLOCK), BLOCK)
            coords_out[:, lanes] = coords
            speeds_out[:, lanes] = speed
            forces_out[:, lanes] = force
        return carry

    lax.fori_loop(0, BLOCKS // 8, step, 0)


def shape(*dims, dtype=f32):
    return jax.ShapeDtypeStruct(dims, dtype)


def pack(scale, send, positions, velocities, charges, solute):
    return pl.pallas_call(
        pack_kernel,
        in_specs=[smem, smem, vmem, vmem, vmem, vmem],
        out_specs=(vmem, vmem),
        out_shape=(shape(BLOCKS, 8, BLOCK), shape(DOMAINS, 8, BLOCK)),
    )(scale, send, positions, velocities, charges, solute)


def place(land, ghost, home, other, states, arrived):
    return pl.pallas_call(
        place_kernel,
        in_specs=[smem, smem, smem, smem, vmem, vmem],
        out_specs=(vmem, vmem),
        out_shape=(shape(BLOCKS + 1, 8, BLOCK), shape(DOMAINS, 2, 5 * BLOCK)),
        scratch_shapes=[pltpu.SMEM((DOMAINS,), jnp.int32)],
    )(land, ghost, home, other, states, arrived)


def local_pairs(home, other, placed):
    return pl.pallas_call(
        local_kernel,
        in_specs=[smem, smem, vmem],
        out_specs=(vmem, vmem),
        out_shape=(shape(BLOCKS, 16, BLOCK), shape(BLOCKS, 32, BLOCK, dtype=bf16)),
        scratch_shapes=[
            pltpu.VMEM((BLOCKS, BLOCK, 64), bf16),
            pltpu.VMEM((BLOCKS, BLOCK, 64), bf16),
            pltpu.VMEM((BLOCKS, 16, BLOCK), bf16),
            pltpu.VMEM((BLOCKS, BLOCK, BLOCK), f32),
        ],
        cost_estimate=pl.CostEstimate(
            flops=1_000_000_000, transcendentals=4_000_000, bytes_accessed=1_000_000
        ),
    )(home, other, placed)


def middle(ghost, home, other, placed, sums, targets, received):
    return pl.pallas_call(
        middle_kernel,
        in_specs=[smem, smem, smem, vmem, vmem, vmem, vmem],
        out_specs=(vmem, vmem),
        out_shape=(shape(BLOCKS + 1, 8, BLOCK), shape(DOMAINS, 2, 3 * BLOCK)),
        scratch_shapes=[
            pltpu.SMEM((DOMAINS,), jnp.int32),
            pltpu.VMEM((BLOCKS, 16, BLOCK), f32),
        ],
    )(ghost, home, other, placed, sums, targets, received)


def last(ghost, home, other, placed, sums, targets, received, earlier):
    flat = shape(3, BLOCKS * BLOCK)
    return pl.pallas_call(
        last_kernel,
        in_specs=[smem, smem, smem, vmem, vmem, vmem, vmem, vmem],
        out_specs=(vmem, vmem, vmem),
        out_shape=(flat, flat, flat),
        scratch_shapes=[
            pltpu.SMEM((DOMAINS,), jnp.int32),
            pltpu.VMEM((BLOCKS, 16, BLOCK), f32),
        ],
    )(ghost, home, other, placed, sums, targets, received, earlier)


def exchange(values):
    return lax.all_to_all(values, "dom", split_axis=0, concat_axis=0, tiled=True)


def on_device(
    positions,
    velocities,
    charges,
    solute,
    rest_scale,
    send_slot,
    land_slot,
    ghost_slot,
    pair_home,
    pair_other,
):
    states, outbound = pack(
        rest_scale,
        send_slot,
        positions,
        velocities,
        charges.reshape(BLOCKS, BLOCK),
        solute.reshape(BLOCKS, BLOCK),
    )
    arrived = exchange(outbound)
    placed, outgoing = place(land_slot, ghost_slot, pair_home, pair_other, states, arrived)
    ghosts = exchange(outgoing)
    sums, targets = local_pairs(pair_home, pair_other, placed)
    placed, outgoing = middle(ghost_slot, pair_home, pair_other, placed, sums, targets, ghosts)
    moved_ghosts = exchange(outgoing)
    sums, targets = local_pairs(pair_home, pair_other, placed)
    return last(
        ghost_slot, pair_home, pair_other, placed, sums, targets, moved_ghosts, ghosts
    )


def solution(mesh):
    in_specs = (
        P(None, ("rep", "dom")),
        P(None, ("rep", "dom")),
        P(("rep", "dom")),
        P(("rep", "dom")),
        P("rep"),
        P(("rep", "dom"), None),
        P(("rep", "dom"), None),
        P(("rep", "dom"), None),
        P(("rep", "dom"), None),
        P(("rep", "dom"), None),
    )
    out_specs = (P(None, ("rep", "dom")), P(None, ("rep", "dom")), P(None, ("rep", "dom")))
    return jax.shard_map(
        on_device, mesh=mesh, in_specs=in_specs, out_specs=out_specs, check_vma=False
    )
```

```python
import math

import jax
import jax.numpy as jnp
from jax import lax
from jax.experimental import pallas as pl
from jax.experimental.pallas import tpu as pltpu
from jax.sharding import PartitionSpec as P

BLOCK = 128
BLOCKS = 64
DOMAINS = 64
LOCAL = 128
LAND, SENT, MATE, HOME, OTHER = range(5)

coupling_scale = 0.2
time_step = 0.05
root_log2e = math.sqrt(math.log2(math.e))
local_unroll = 32
ghost_unroll = 32
f32 = jnp.float32
bf16 = jnp.bfloat16

vmem = pl.BlockSpec(memory_space=pltpu.VMEM)
smem = pl.BlockSpec(memory_space=pltpu.SMEM)


def rounded(values):
    return values.astype(bf16).astype(f32)


def split3(values):
    first = rounded(values)
    rest = values - first
    second = rounded(rest)
    return first, second, rounded(rest - second)


def exponent_parts(coords):
    scaled = coords * root_log2e
    half = 0.5 * jnp.sum(scaled * scaled, 0, keepdims=True)
    return split3(jnp.concatenate([scaled, half, scaled, half], 0))


def row_masks():
    row = lax.broadcasted_iota(jnp.int32, (8, BLOCK), 0)
    return row == 3, row == 7, row < 4


def source_rows(parts, charge):
    p0, p1, p2 = parts
    third, last, low = row_masks()
    s0 = jnp.where(third, -p0, jnp.where(last, -p1, p0))
    s1 = jnp.where(third, -p2, jnp.where(last, 1.0, p1))
    s2 = jnp.where(third | last, 1.0, jnp.where(low, p0, p2))
    return jnp.concatenate([s0, s1, s2, jnp.broadcast_to(charge, (8, BLOCK))], 0)


def target_rows(parts):
    p0, p1, p2 = parts
    third, last, low = row_masks()
    t0 = jnp.where(third | last, 1.0, jnp.where(low, p0, p1))
    t1 = jnp.where(third, 1.0, jnp.where(last, -p0, jnp.where(low, p0, p1)))
    t2 = jnp.where(third, -p1, jnp.where(last, -p2, jnp.where(low, p2, p0)))
    return jnp.concatenate([t0, t1, t2, jnp.zeros((8, BLOCK), f32)], 0).astype(bf16)


def weight_rows(coords, weight):
    low = row_masks()[2]
    ones = jnp.ones((1, BLOCK), f32)
    w0, w1, w2 = split3(jnp.concatenate([coords, ones, coords, ones], 0) * weight)
    return jnp.concatenate([jnp.where(low, w0, w1), jnp.where(low, w2, 0.0)], 0).astype(bf16)


def coupled_sums(sources, charges, weights, targets, target_charges):
    empty = jnp.zeros((32, BLOCK), bf16)
    right = jnp.concatenate(
        [
            jnp.concatenate([targets[0], empty], 1),
            jnp.concatenate([empty, targets[1]], 1),
        ],
        0,
    )
    exponent = jnp.dot(sources, right, preferred_element_type=f32)
    tiles = []
    for which in range(2):
        decay = jnp.exp2(exponent[:, which * BLOCK : (which + 1) * BLOCK])
        tiles.append(decay * (charges[which] * target_charges[which] + decay))
    coupling = jnp.concatenate(tiles, 1)
    high = coupling.astype(bf16)
    low = (coupling - high.astype(f32)).astype(bf16)
    stacked = jnp.concatenate([high, low], 0)
    left = jnp.concatenate(weights, 0)
    left = jnp.concatenate([left, left], 1)
    return jnp.dot(left, stacked, preferred_element_type=f32)


def pack_kernel(scale, send, positions, velocities, charges, solute, states, outbound):
    root = jnp.sqrt(jnp.full((8, BLOCK), scale[0], f32))

    def gather(group, carry):
        first = pl.multiple_of(group * 8, 8)
        charge_rows = charges[pl.ds(first, 8), :]
        weight = jnp.where(solute[pl.ds(first, 8), :] == 1, root, 1.0)
        for inner in range(8):
            lanes = pl.ds(pl.multiple_of((group * 8 + inner) * BLOCK, BLOCK), BLOCK)
            states[group * 8 + inner] = jnp.concatenate(
                [
                    positions[:, lanes],
                    velocities[:, lanes],
                    charge_rows[inner : inner + 1],
                    weight[inner : inner + 1],
                ],
                0,
            )
        return carry

    lax.fori_loop(0, BLOCKS // 8, gather, 0)

    def hand_over(group, carry):
        for inner in range(8):
            peer = group * 8 + inner
            outbound[peer] = states[jnp.minimum(send[0, peer], BLOCKS - 1)]
        return carry

    lax.fori_loop(0, DOMAINS // 8, hand_over, 0)


def table_kernel(land, ghost, home, other, table):
    def by_peer(peer, carry):
        table[LAND, peer] = land[0, peer]
        table[SENT, peer] = ghost[0, peer]
        table[MATE, other[0, LOCAL + peer] - BLOCKS] = home[0, LOCAL + peer]
        return carry

    lax.fori_loop(0, DOMAINS, by_peer, 0)

    def by_pair(entry, carry):
        table[HOME, entry] = home[0, entry]
        table[OTHER, entry] = other[0, entry]
        return carry

    lax.fori_loop(0, LOCAL, by_pair, 0)


def place_kernel(table, states, arrived, placed, outgoing):
    def keep(group, carry):
        placed[pl.ds(group * 8, 8)] = states[pl.ds(group * 8, 8)]
        return carry

    lax.fori_loop(0, BLOCKS // 8, keep, 0)

    def receive(group, carry):
        for inner in range(8):
            peer = group * 8 + inner
            placed[table[LAND, peer]] = arrived[peer]
        return carry

    lax.fori_loop(0, DOMAINS // 8, receive, 0)

    def send(group, carry):
        for inner in range(8):
            peer = group * 8 + inner
            for which, slot in enumerate((table[SENT, peer], table[MATE, peer])):
                for column, row in enumerate((0, 1, 2, 6, 7)):
                    outgoing[peer, which : which + 1, column * BLOCK : (column + 1) * BLOCK] = (
                        placed[slot, row : row + 1, :]
                    )
        return carry

    lax.fori_loop(0, DOMAINS // 8, send, 0)


def local_kernel(table, placed, sums, targets, first, second, weights, spread):
    def prepare(group):
        stacked = []
        for inner in range(4):
            block = group * 4 + inner
            state = placed[block]
            parts = exponent_parts(state[0:3])
            targets[block] = target_rows(parts)
            weights[block] = weight_rows(state[0:3], state[7:8])
            stacked.append(source_rows(parts, state[6:7]))
            sums[block] = jnp.zeros((16, BLOCK), f32)
        columns = jnp.concatenate(stacked, 0).T
        empty = jnp.zeros((BLOCK, 32), bf16)
        for inner in range(4):
            block = group * 4 + inner
            chosen = columns[:, inner * 32 : (inner + 1) * 32]
            narrow = chosen.astype(bf16)
            first[block] = jnp.concatenate([narrow, empty], 1)
            second[block] = jnp.concatenate([empty, narrow], 1)
            spread[block] = jnp.broadcast_to(chosen[:, 24:25], (BLOCK, BLOCK))

    def prepare_some(chunk, carry):
        for inner in range(4):
            prepare(chunk * 4 + inner)
        return carry

    lax.fori_loop(0, BLOCKS // 16, prepare_some, 0)

    def pairs(group, carry):
        for inner in range(local_unroll):
            entry = group * local_unroll + inner
            one = table[HOME, entry]
            two = table[OTHER, entry]
            result = coupled_sums(
                first[two] + second[one],
                (spread[two], spread[one]),
                (weights[two], weights[one]),
                (targets[one], targets[two]),
                (placed[one, 6:7, :], placed[two, 6:7, :]),
            )
            sums[one] += result[:16, :BLOCK]
            sums[two] += result[16:, BLOCK:]
        return carry

    lax.fori_loop(0, LOCAL // local_unroll, pairs, 0)


def ghost_pairs(table, placed, targets, sums, total, coords_of, params_of):
    def start(group, carry):
        total[pl.ds(group * 8, 8)] = sums[pl.ds(group * 8, 8)]
        return carry

    lax.fori_loop(0, BLOCKS // 8, start, 0)

    def pairs(group, carry):
        for half in range(ghost_unroll // 2):
            stacked = []
            weights = []
            for inner in range(2):
                peer = group * ghost_unroll + half * 2 + inner
                for which in range(2):
                    coords = coords_of(peer, which)
                    charge, weight = params_of(peer, which)
                    stacked.append(source_rows(exponent_parts(coords), charge))
                    weights.append(weight_rows(coords, weight))
            columns = jnp.concatenate(stacked, 0).T
            narrow = columns.astype(bf16)
            for inner in range(2):
                peer = group * ghost_unroll + half * 2 + inner
                one = table[MATE, peer]
                two = table[SENT, peer]
                lane = inner * 64
                result = coupled_sums(
                    narrow[:, lane : lane + 64],
                    (
                        jnp.broadcast_to(columns[:, lane + 24 : lane + 25], (BLOCK, BLOCK)),
                        jnp.broadcast_to(columns[:, lane + 56 : lane + 57], (BLOCK, BLOCK)),
                    ),
                    (weights[inner * 2], weights[inner * 2 + 1]),
                    (targets[one], targets[two]),
                    (placed[one, 6:7, :], placed[two, 6:7, :]),
                )
                total[one] += result[:16, :BLOCK]
                total[two] += result[16:, BLOCK:]
        return carry

    lax.fori_loop(0, DOMAINS // ghost_unroll, pairs, 0)


def moved(state, total):
    folded = total[0:4] + total[4:8] + total[8:12]
    force = (coupling_scale * state[7:8]) * (state[0:3] * folded[3:4] - folded[0:3])
    speed = state[3:6] + time_step * force
    return state[0:3] + time_step * speed, speed, force


def middle_kernel(table, placed, sums, targets, received, updated, outgoing, total):
    def row(peer, which, column):
        return received[peer, which : which + 1, column * BLOCK : (column + 1) * BLOCK]

    ghost_pairs(
        table,
        placed,
        targets,
        sums,
        total,
        lambda peer, which: jnp.concatenate([row(peer, which, c) for c in range(3)], 0),
        lambda peer, which: (row(peer, which, 3), row(peer, which, 4)),
    )

    def step(group, carry):
        for inner in range(8):
            block = group * 8 + inner
            state = placed[block]
            coords, speed, _ = moved(state, total[block])
            updated[block] = jnp.concatenate([coords, speed, state[6:8]], 0)
        return carry

    lax.fori_loop(0, BLOCKS // 8, step, 0)

    def send(group, carry):
        for inner in range(8):
            peer = group * 8 + inner
            for which, slot in enumerate((table[SENT, peer], table[MATE, peer])):
                for column in range(3):
                    outgoing[peer, which : which + 1, column * BLOCK : (column + 1) * BLOCK] = (
                        updated[slot, column : column + 1, :]
                    )
        return carry

    lax.fori_loop(0, DOMAINS // 8, send, 0)


def last_kernel(
    table,
    placed,
    sums,
    targets,
    received,
    earlier,
    coords_out,
    speeds_out,
    forces_out,
    total,
):
    def row(ref, peer, which, column):
        return ref[peer, which : which + 1, column * BLOCK : (column + 1) * BLOCK]

    ghost_pairs(
        table,
        placed,
        targets,
        sums,
        total,
        lambda peer, which: jnp.concatenate([row(received, peer, which, c) for c in range(3)], 0),
        lambda peer, which: (row(earlier, peer, which, 3), row(earlier, peer, which, 4)),
    )

    def step(group, carry):
        for inner in range(8):
            block = group * 8 + inner
            coords, speed, force = moved(placed[block], total[block])
            lanes = pl.ds(pl.multiple_of(block * BLOCK, BLOCK), BLOCK)
            coords_out[:, lanes] = coords
            speeds_out[:, lanes] = speed
            forces_out[:, lanes] = force
        return carry

    lax.fori_loop(0, BLOCKS // 8, step, 0)


def grant(mebibytes):
    return pltpu.CompilerParams(vmem_limit_bytes=mebibytes << 20)


def shape(*dims, dtype=f32):
    return jax.ShapeDtypeStruct(dims, dtype)


def in_hbm(values):
    return pltpu.with_memory_space_constraint(values, pltpu.HBM)


def pack(scale, send, positions, velocities, charges, solute):
    return pl.pallas_call(
        pack_kernel,
        compiler_params=grant(4),
        in_specs=[smem, smem, vmem, vmem, vmem, vmem],
        out_specs=(vmem, vmem),
        out_shape=(shape(BLOCKS, 8, BLOCK), shape(DOMAINS, 8, BLOCK)),
    )(scale, send, *(in_hbm(x) for x in (positions, velocities, charges, solute)))


def tables(land, ghost, home, other):
    return pl.pallas_call(
        table_kernel,
        compiler_params=grant(1),
        in_specs=[smem, smem, smem, smem],
        out_specs=smem,
        out_shape=shape(8, LOCAL, dtype=jnp.int32),
        cost_estimate=pl.CostEstimate(
            flops=100_000_000, transcendentals=0, bytes_accessed=10_000
        ),
    )(land, ghost, home, other)


def place(table, states, arrived):
    return pl.pallas_call(
        place_kernel,
        compiler_params=grant(4),
        in_specs=[smem, vmem, vmem],
        out_specs=(vmem, vmem),
        out_shape=(shape(BLOCKS + 1, 8, BLOCK), shape(DOMAINS, 2, 5 * BLOCK)),
    )(table, states, arrived)


def local_pairs(table, placed):
    return pl.pallas_call(
        local_kernel,
        compiler_params=grant(16),
        in_specs=[smem, vmem],
        out_specs=(vmem, vmem),
        out_shape=(shape(BLOCKS, 16, BLOCK), shape(BLOCKS, 32, BLOCK, dtype=bf16)),
        scratch_shapes=[
            pltpu.VMEM((BLOCKS, BLOCK, 64), bf16),
            pltpu.VMEM((BLOCKS, BLOCK, 64), bf16),
            pltpu.VMEM((BLOCKS, 16, BLOCK), bf16),
            pltpu.VMEM((BLOCKS, BLOCK, BLOCK), f32),
        ],
        cost_estimate=pl.CostEstimate(
            flops=1_000_000_000, transcendentals=4_000_000, bytes_accessed=1_000_000
        ),
    )(table, placed)


def middle(table, placed, sums, targets, received):
    return pl.pallas_call(
        middle_kernel,
        compiler_params=grant(8),
        in_specs=[smem, vmem, vmem, vmem, vmem],
        out_specs=(vmem, vmem),
        out_shape=(shape(BLOCKS + 1, 8, BLOCK), shape(DOMAINS, 2, 3 * BLOCK)),
        scratch_shapes=[
            pltpu.VMEM((BLOCKS, 16, BLOCK), f32),
        ],
    )(table, placed, sums, targets, received)


def last(table, placed, sums, targets, received, earlier):
    flat = shape(3, BLOCKS * BLOCK)
    return pl.pallas_call(
        last_kernel,
        compiler_params=grant(8),
        in_specs=[smem, vmem, vmem, vmem, vmem, vmem],
        out_specs=(vmem, vmem, vmem),
        out_shape=(flat, flat, flat),
        scratch_shapes=[
            pltpu.VMEM((BLOCKS, 16, BLOCK), f32),
        ],
    )(table, placed, sums, targets, received, earlier)


def exchange(values):
    return lax.all_to_all(values, "dom", split_axis=0, concat_axis=0, tiled=True)


def on_device(
    positions,
    velocities,
    charges,
    solute,
    rest_scale,
    send_slot,
    land_slot,
    ghost_slot,
    pair_home,
    pair_other,
):
    states, outbound = pack(
        rest_scale,
        send_slot,
        positions,
        velocities,
        charges.reshape(BLOCKS, BLOCK),
        solute.reshape(BLOCKS, BLOCK),
    )
    arrived = exchange(outbound)
    table = tables(land_slot, ghost_slot, pair_home, pair_other)
    placed, outgoing = place(table, states, arrived)
    ghosts = exchange(outgoing)
    sums, targets = local_pairs(table, placed)
    placed, outgoing = middle(table, placed, sums, targets, ghosts)
    moved_ghosts = exchange(outgoing)
    sums, targets = local_pairs(table, placed)
    return last(table, placed, sums, targets, moved_ghosts, ghosts)


def solution(mesh):
    in_specs = (
        P(None, ("rep", "dom")),
        P(None, ("rep", "dom")),
        P(("rep", "dom")),
        P(("rep", "dom")),
        P("rep"),
        P(("rep", "dom"), None),
        P(("rep", "dom"), None),
        P(("rep", "dom"), None),
        P(("rep", "dom"), None),
        P(("rep", "dom"), None),
    )
    out_specs = (P(None, ("rep", "dom")), P(None, ("rep", "dom")), P(None, ("rep", "dom")))
    return jax.shard_map(
        on_device, mesh=mesh, in_specs=in_specs, out_specs=out_specs, check_vma=False
    )
```

```python
import math

import jax
import jax.numpy as jnp
from jax import lax
from jax.experimental import pallas as pl
from jax.experimental.pallas import tpu as pltpu
from jax.sharding import PartitionSpec as P

BLOCK = 128
HALF = BLOCK // 2
BLOCKS = 64
DOMAINS = 64
LOCAL = 128

coupling_scale = 0.2
time_step = 0.05
root_log2e = math.sqrt(math.log2(math.e))
local_unroll = 128
ghost_unroll = 64
f32 = jnp.float32
bf16 = jnp.bfloat16

vmem = pl.BlockSpec(memory_space=pltpu.VMEM)
smem = pl.BlockSpec(memory_space=pltpu.SMEM)


def rounded(values):
    return values.astype(bf16).astype(f32)


def split3(values):
    first = rounded(values)
    rest = values - first
    second = rounded(rest)
    return first, second, rounded(rest - second)


def exponent_parts(coords):
    scaled = coords * root_log2e
    half = 0.5 * jnp.sum(scaled * scaled, 0, keepdims=True)
    return split3(jnp.concatenate([scaled, half, scaled, half], 0))


def row_masks():
    row = lax.broadcasted_iota(jnp.int32, (8, BLOCK), 0)
    return row == 3, row == 7, row < 4


def source_rows(parts, charge):
    p0, p1, p2 = parts
    third, last, low = row_masks()
    s0 = jnp.where(third, -p0, jnp.where(last, -p1, p0))
    s1 = jnp.where(third, -p2, jnp.where(last, 1.0, p1))
    s2 = jnp.where(third | last, 1.0, jnp.where(low, p0, p2))
    return jnp.concatenate([s0, s1, s2, jnp.broadcast_to(charge, (8, BLOCK))], 0)


def target_rows(parts):
    p0, p1, p2 = parts
    third, last, low = row_masks()
    t0 = jnp.where(third | last, 1.0, jnp.where(low, p0, p1))
    t1 = jnp.where(third, 1.0, jnp.where(last, -p0, jnp.where(low, p0, p1)))
    t2 = jnp.where(third, -p1, jnp.where(last, -p2, jnp.where(low, p2, p0)))
    return jnp.concatenate([t0, t1, t2, jnp.zeros((8, BLOCK), f32)], 0).astype(bf16)


def weight_rows(coords, weight):
    low = row_masks()[2]
    ones = jnp.ones((1, BLOCK), f32)
    w0, w1, w2 = split3(jnp.concatenate([coords, ones, coords, ones], 0) * weight)
    rows = jnp.concatenate([jnp.where(low, w0, w1), jnp.where(low, w2, 0.0)], 0)
    turned = pltpu.roll(rows, HALF, 1)
    early = lax.broadcasted_iota(jnp.int32, (16, BLOCK), 1) < HALF
    return jnp.concatenate(
        [jnp.where(early, rows, turned), jnp.where(early, turned, rows)], 1
    ).astype(bf16)


def coupled_sums(sources, charges, weights, targets, target_charges):
    depth = sources.shape[1] // 2
    empty = jnp.zeros((32, BLOCK), bf16)
    right = [
        jnp.concatenate([targets[0], empty], 1),
        jnp.concatenate([empty, targets[1]], 1),
    ]
    if depth > 32:
        gap = jnp.zeros((depth - 32, 2 * BLOCK), bf16)
        right = [right[0], gap, right[1], gap]
    exponent = jnp.dot(sources, jnp.concatenate(right, 0), preferred_element_type=f32)
    tiles = []
    for which in range(2):
        decay = jnp.exp2(exponent[:, which * BLOCK : (which + 1) * BLOCK])
        tiles.append(decay * (charges[which] * target_charges[which] + decay))
    coupling = jnp.concatenate(tiles, 1)
    high = coupling.astype(bf16)
    low = (coupling - high.astype(f32)).astype(bf16)
    stacked = jnp.concatenate([high[:HALF], low[:HALF], high[HALF:], low[HALF:]], 0)
    left = jnp.concatenate(weights, 0)
    return jnp.dot(left, stacked, preferred_element_type=f32)


def pack_kernel(scale, send, positions, velocities, charges, solute, states, outbound):
    root = jnp.sqrt(jnp.full((8, BLOCK), scale[0], f32))

    def gather(group, carry):
        first = pl.multiple_of(group * 8, 8)
        charge_rows = charges[pl.ds(first, 8), :]
        weight = jnp.where(solute[pl.ds(first, 8), :] == 1, root, 1.0)
        for inner in range(8):
            lanes = pl.ds(pl.multiple_of((group * 8 + inner) * BLOCK, BLOCK), BLOCK)
            states[group * 8 + inner] = jnp.concatenate(
                [
                    positions[:, lanes],
                    velocities[:, lanes],
                    charge_rows[inner : inner + 1],
                    weight[inner : inner + 1],
                ],
                0,
            )
        return carry

    lax.fori_loop(0, BLOCKS // 8, gather, 0)

    def hand_over(group, carry):
        for inner in range(8):
            peer = group * 8 + inner
            outbound[peer] = states[jnp.minimum(send[0, peer], BLOCKS - 1)]
        return carry

    lax.fori_loop(0, DOMAINS // 8, hand_over, 0)


def table_kernel(land, ghost, home, other, local_table, ghost_table):
    def by_pair(group, carry):
        for inner in range(8):
            entry = group * 8 + inner
            local_table[0, entry] = home[0, entry] + BLOCKS * other[0, entry]
        return carry

    lax.fori_loop(0, LOCAL // 8, by_pair, 0)

    def by_peer(group, carry):
        for inner in range(8):
            entry = LOCAL + group * 8 + inner
            peer = other[0, entry] - BLOCKS
            ghost_table[0, peer] = home[0, entry] + BLOCKS * (ghost[0, peer] + BLOCKS * land[0, peer])
        return carry

    lax.fori_loop(0, DOMAINS // 8, by_peer, 0)


def pair_of(table, entry):
    packed = table[0, entry]
    return packed & (BLOCKS - 1), (packed >> 6) & (BLOCKS - 1)


def place_kernel(table, states, arrived, placed, outgoing):
    def keep(group, carry):
        placed[pl.ds(group * 8, 8)] = states[pl.ds(group * 8, 8)]
        return carry

    lax.fori_loop(0, BLOCKS // 8, keep, 0)

    def receive(group, carry):
        for inner in range(8):
            peer = group * 8 + inner
            placed[table[0, peer] >> 12] = arrived[peer]
        return carry

    lax.fori_loop(0, DOMAINS // 8, receive, 0)

    def send(group, carry):
        for inner in range(8):
            peer = group * 8 + inner
            mate, sent = pair_of(table, peer)
            for which, slot in enumerate((sent, mate)):
                for column, row in enumerate((0, 1, 2, 6, 7)):
                    outgoing[peer, which : which + 1, column * BLOCK : (column + 1) * BLOCK] = (
                        placed[slot, row : row + 1, :]
                    )
        return carry

    lax.fori_loop(0, DOMAINS // 8, send, 0)


def local_kernel(table, placed, sums, targets, columns_of, weights, spread):
    def prepare(group):
        stacked = []
        for inner in range(4):
            block = group * 4 + inner
            state = placed[block]
            parts = exponent_parts(state[0:3])
            targets[block] = target_rows(parts)
            weights[block] = weight_rows(state[0:3], state[7:8])
            stacked.append(source_rows(parts, state[6:7]))
            sums[block] = jnp.zeros((16, BLOCK), f32)
        columns = jnp.concatenate(stacked, 0).T
        empty = jnp.zeros((BLOCK, BLOCK - 32), bf16)
        for inner in range(4):
            block = group * 4 + inner
            chosen = columns[:, inner * 32 : (inner + 1) * 32]
            columns_of[block] = jnp.concatenate([chosen.astype(bf16), empty], 1)
            spread[block] = jnp.broadcast_to(chosen[:, 24:25], (BLOCK, BLOCK))

    def prepare_some(chunk, carry):
        for inner in range(4):
            prepare(chunk * 4 + inner)
        return carry

    lax.fori_loop(0, BLOCKS // 16, prepare_some, 0)

    def pairs(group, carry):
        for inner in range(local_unroll):
            entry = group * local_unroll + inner
            one, two = pair_of(table, entry)
            result = coupled_sums(
                jnp.concatenate([columns_of[two], columns_of[one]], 1),
                (spread[two], spread[one]),
                (weights[two], weights[one]),
                (targets[one], targets[two]),
                (placed[one, 6:7, :], placed[two, 6:7, :]),
            )
            sums[one] += result[:16, :BLOCK]
            sums[two] += result[16:, BLOCK:]
        return carry

    lax.fori_loop(0, LOCAL // local_unroll, pairs, 0)


def ghost_pairs(table, placed, targets, sums, total, coords_of, params_of):
    def start(group, carry):
        total[pl.ds(group * 8, 8)] = sums[pl.ds(group * 8, 8)]
        return carry

    lax.fori_loop(0, BLOCKS // 8, start, 0)

    def pairs(group, carry):
        for half in range(ghost_unroll // 2):
            stacked = []
            weights = []
            for inner in range(2):
                peer = group * ghost_unroll + half * 2 + inner
                for which in range(2):
                    coords = coords_of(peer, which)
                    charge, weight = params_of(peer, which)
                    stacked.append(source_rows(exponent_parts(coords), charge))
                    weights.append(weight_rows(coords, weight))
            columns = jnp.concatenate(stacked, 0).T
            narrow = columns.astype(bf16)
            for inner in range(2):
                peer = group * ghost_unroll + half * 2 + inner
                one, two = pair_of(table, peer)
                lane = inner * 64
                result = coupled_sums(
                    narrow[:, lane : lane + 64],
                    (
                        jnp.broadcast_to(columns[:, lane + 24 : lane + 25], (BLOCK, BLOCK)),
                        jnp.broadcast_to(columns[:, lane + 56 : lane + 57], (BLOCK, BLOCK)),
                    ),
                    (weights[inner * 2], weights[inner * 2 + 1]),
                    (targets[one], targets[two]),
                    (placed[one, 6:7, :], placed[two, 6:7, :]),
                )
                total[one] += result[:16, :BLOCK]
                total[two] += result[16:, BLOCK:]
        return carry

    lax.fori_loop(0, DOMAINS // ghost_unroll, pairs, 0)


def moved(state, total):
    folded = total[0:4] + total[4:8] + total[8:12]
    force = (coupling_scale * state[7:8]) * (state[0:3] * folded[3:4] - folded[0:3])
    speed = state[3:6] + time_step * force
    return state[0:3] + time_step * speed, speed, force


def middle_kernel(table, placed, sums, targets, received, updated, outgoing, total):
    def row(peer, which, column):
        return received[peer, which : which + 1, column * BLOCK : (column + 1) * BLOCK]

    ghost_pairs(
        table,
        placed,
        targets,
        sums,
        total,
        lambda peer, which: jnp.concatenate([row(peer, which, c) for c in range(3)], 0),
        lambda peer, which: (row(peer, which, 3), row(peer, which, 4)),
    )

    def step(group, carry):
        for inner in range(8):
            block = group * 8 + inner
            state = placed[block]
            coords, speed, _ = moved(state, total[block])
            updated[block] = jnp.concatenate([coords, speed, state[6:8]], 0)
        return carry

    lax.fori_loop(0, BLOCKS // 8, step, 0)

    def send(group, carry):
        for inner in range(8):
            peer = group * 8 + inner
            mate, sent = pair_of(table, peer)
            for which, slot in enumerate((sent, mate)):
                for column in range(3):
                    outgoing[peer, which : which + 1, column * BLOCK : (column + 1) * BLOCK] = (
                        updated[slot, column : column + 1, :]
                    )
        return carry

    lax.fori_loop(0, DOMAINS // 8, send, 0)


def last_kernel(
    table,
    placed,
    sums,
    targets,
    received,
    earlier,
    coords_out,
    speeds_out,
    forces_out,
    total,
):
    def row(ref, peer, which, column):
        return ref[peer, which : which + 1, column * BLOCK : (column + 1) * BLOCK]

    ghost_pairs(
        table,
        placed,
        targets,
        sums,
        total,
        lambda peer, which: jnp.concatenate([row(received, peer, which, c) for c in range(3)], 0),
        lambda peer, which: (row(earlier, peer, which, 3), row(earlier, peer, which, 4)),
    )

    def step(group, carry):
        for inner in range(8):
            block = group * 8 + inner
            coords, speed, force = moved(placed[block], total[block])
            lanes = pl.ds(pl.multiple_of(block * BLOCK, BLOCK), BLOCK)
            coords_out[:, lanes] = coords
            speeds_out[:, lanes] = speed
            forces_out[:, lanes] = force
        return carry

    lax.fori_loop(0, BLOCKS // 8, step, 0)


def grant(mebibytes):
    return pltpu.CompilerParams(vmem_limit_bytes=mebibytes << 20)


def shape(*dims, dtype=f32):
    return jax.ShapeDtypeStruct(dims, dtype)


def in_hbm(values):
    return pltpu.with_memory_space_constraint(values, pltpu.HBM)


def pack(scale, send, positions, velocities, charges, solute):
    return pl.pallas_call(
        pack_kernel,
        compiler_params=grant(4),
        in_specs=[smem, smem, vmem, vmem, vmem, vmem],
        out_specs=(vmem, vmem),
        out_shape=(shape(BLOCKS, 8, BLOCK), shape(DOMAINS, 8, BLOCK)),
    )(scale, *(in_hbm(x) for x in (send, positions, velocities, charges, solute)))


def tables(land, ghost, home, other):
    return pl.pallas_call(
        table_kernel,
        compiler_params=grant(1),
        in_specs=[smem, smem, smem, smem],
        out_specs=(smem, smem),
        out_shape=(shape(1, LOCAL, dtype=jnp.int32), shape(1, DOMAINS, dtype=jnp.int32)),
        cost_estimate=pl.CostEstimate(
            flops=100_000_000, transcendentals=0, bytes_accessed=10_000
        ),
    )(land, ghost, home, other)


def place(table, states, arrived):
    return pl.pallas_call(
        place_kernel,
        compiler_params=grant(4),
        in_specs=[smem, vmem, vmem],
        out_specs=(vmem, vmem),
        out_shape=(shape(BLOCKS + 1, 8, BLOCK), shape(DOMAINS, 2, 5 * BLOCK)),
    )(table, states, arrived)


def local_pairs(table, placed):
    return pl.pallas_call(
        local_kernel,
        compiler_params=grant(16),
        in_specs=[smem, vmem],
        out_specs=(vmem, vmem),
        out_shape=(shape(BLOCKS, 16, BLOCK), shape(BLOCKS, 32, BLOCK, dtype=bf16)),
        scratch_shapes=[
            pltpu.VMEM((BLOCKS, BLOCK, BLOCK), bf16),
            pltpu.VMEM((BLOCKS, 16, 2 * BLOCK), bf16),
            pltpu.VMEM((BLOCKS, BLOCK, BLOCK), f32),
        ],
        cost_estimate=pl.CostEstimate(
            flops=1_000_000_000, transcendentals=4_000_000, bytes_accessed=1_000_000
        ),
    )(table, placed)


def middle(table, placed, sums, targets, received):
    return pl.pallas_call(
        middle_kernel,
        compiler_params=grant(8),
        in_specs=[smem, vmem, vmem, vmem, vmem],
        out_specs=(vmem, vmem),
        out_shape=(shape(BLOCKS + 1, 8, BLOCK), shape(DOMAINS, 2, 3 * BLOCK)),
        scratch_shapes=[
            pltpu.VMEM((BLOCKS, 16, BLOCK), f32),
        ],
    )(table, placed, sums, targets, received)


def last(table, placed, sums, targets, received, earlier):
    flat = shape(3, BLOCKS * BLOCK)
    return pl.pallas_call(
        last_kernel,
        compiler_params=grant(8),
        in_specs=[smem, vmem, vmem, vmem, vmem, vmem],
        out_specs=(vmem, vmem, vmem),
        out_shape=(flat, flat, flat),
        scratch_shapes=[
            pltpu.VMEM((BLOCKS, 16, BLOCK), f32),
        ],
    )(table, placed, sums, targets, received, earlier)


def exchange(values):
    return lax.all_to_all(values, "dom", split_axis=0, concat_axis=0, tiled=True)


def on_device(
    positions,
    velocities,
    charges,
    solute,
    rest_scale,
    send_slot,
    land_slot,
    ghost_slot,
    pair_home,
    pair_other,
):
    states, outbound = pack(
        rest_scale,
        send_slot,
        positions,
        velocities,
        charges.reshape(BLOCKS, BLOCK),
        solute.reshape(BLOCKS, BLOCK),
    )
    arrived = exchange(outbound)
    local_table, ghost_table = tables(land_slot, ghost_slot, pair_home, pair_other)
    placed, outgoing = place(ghost_table, states, arrived)
    ghosts = exchange(outgoing)
    sums, targets = local_pairs(local_table, placed)
    placed, outgoing = middle(ghost_table, placed, sums, targets, ghosts)
    moved_ghosts = exchange(outgoing)
    sums, targets = local_pairs(local_table, placed)
    return last(ghost_table, placed, sums, targets, moved_ghosts, ghosts)


def solution(mesh):
    in_specs = (
        P(None, ("rep", "dom")),
        P(None, ("rep", "dom")),
        P(("rep", "dom")),
        P(("rep", "dom")),
        P("rep"),
        P(("rep", "dom"), None),
        P(("rep", "dom"), None),
        P(("rep", "dom"), None),
        P(("rep", "dom"), None),
        P(("rep", "dom"), None),
    )
    out_specs = (P(None, ("rep", "dom")), P(None, ("rep", "dom")), P(None, ("rep", "dom")))
    return jax.shard_map(
        on_device, mesh=mesh, in_specs=in_specs, out_specs=out_specs, check_vma=False
    )
```

```python
import math

import jax
import jax.numpy as jnp
from jax import lax
from jax.experimental import pallas as pl
from jax.experimental.pallas import tpu as pltpu
from jax.sharding import PartitionSpec as P

BLOCK = 128
BLOCKS = 64
DOMAINS = 64
LOCAL = 128

coupling_scale = 0.2
time_step = 0.05
root_log2e = math.sqrt(math.log2(math.e))
local_unroll = 128
ghost_unroll = 64
f32 = jnp.float32
bf16 = jnp.bfloat16

vmem = pl.BlockSpec(memory_space=pltpu.VMEM)
smem = pl.BlockSpec(memory_space=pltpu.SMEM)


def repeat(count, body):
    for index in range(count):
        body(index, 0)


def rounded(values):
    return values.astype(bf16).astype(f32)


def split3(values):
    first = rounded(values)
    rest = values - first
    second = rounded(rest)
    return first, second, rounded(rest - second)


def exponent_parts(coords):
    scaled = coords * root_log2e
    half = 0.5 * jnp.sum(scaled * scaled, 0, keepdims=True)
    return split3(jnp.concatenate([scaled, half, scaled, half], 0))


def row_masks():
    row = lax.broadcasted_iota(jnp.int32, (8, BLOCK), 0)
    return row == 3, row == 7, row < 4


def source_rows(parts, charge):
    p0, p1, p2 = parts
    third, last, low = row_masks()
    s0 = jnp.where(third, -p0, jnp.where(last, -p1, p0))
    s1 = jnp.where(third, -p2, jnp.where(last, 1.0, p1))
    s2 = jnp.where(third | last, 1.0, jnp.where(low, p0, p2))
    return jnp.concatenate([s0, s1, s2, jnp.broadcast_to(charge, (8, BLOCK))], 0)


def target_rows(parts):
    p0, p1, p2 = parts
    third, last, low = row_masks()
    t0 = jnp.where(third | last, 1.0, jnp.where(low, p0, p1))
    t1 = jnp.where(third, 1.0, jnp.where(last, -p0, jnp.where(low, p0, p1)))
    t2 = jnp.where(third, -p1, jnp.where(last, -p2, jnp.where(low, p2, p0)))
    return jnp.concatenate([t0, t1, t2, jnp.zeros((8, BLOCK), f32)], 0).astype(bf16)


def weight_rows(coords, weight):
    low = row_masks()[2]
    ones = jnp.ones((1, BLOCK), f32)
    w0, w1, w2 = split3(jnp.concatenate([coords, ones, coords, ones], 0) * weight)
    return jnp.concatenate([jnp.where(low, w0, w1), jnp.where(low, w2, 0.0)], 0).astype(bf16)


def coupled_sums(sources, charges, weights, targets, target_charges):
    depth = sources.shape[1] // 2
    empty = jnp.zeros((32, BLOCK), bf16)
    right = [
        jnp.concatenate([targets[0], empty], 1),
        jnp.concatenate([empty, targets[1]], 1),
    ]
    if depth > 32:
        gap = jnp.zeros((depth - 32, 2 * BLOCK), bf16)
        right = [right[0], gap, right[1], gap]
    exponent = jnp.dot(sources, jnp.concatenate(right, 0), preferred_element_type=f32)
    tiles = []
    for which in range(2):
        decay = jnp.exp2(exponent[:, which * BLOCK : (which + 1) * BLOCK])
        tiles.append(decay * (charges[which] * target_charges[which] + decay))
    coupling = jnp.concatenate(tiles, 1)
    high = coupling.astype(bf16)
    low = (coupling - high.astype(f32)).astype(bf16)
    stacked = jnp.concatenate([high, low], 0)
    left = jnp.concatenate(weights, 0)
    left = jnp.concatenate([left, left], 1)
    return jnp.dot(left, stacked, preferred_element_type=f32)


def pack_kernel(scale, send, positions, velocities, charges, solute, states, outbound):
    root = jnp.sqrt(jnp.full((8, BLOCK), scale[0], f32))

    def gather(group, carry):
        first = group * 8
        charge_rows = charges[pl.ds(first, 8), :]
        weight = jnp.where(solute[pl.ds(first, 8), :] == 1, root, 1.0)
        for inner in range(8):
            lanes = pl.ds((group * 8 + inner) * BLOCK, BLOCK)
            states[group * 8 + inner] = jnp.concatenate(
                [
                    positions[:, lanes],
                    velocities[:, lanes],
                    charge_rows[inner : inner + 1],
                    weight[inner : inner + 1],
                ],
                0,
            )
        return carry

    repeat(BLOCKS // 8, gather)

    def hand_over(group, carry):
        for inner in range(8):
            peer = group * 8 + inner
            outbound[peer] = states[jnp.minimum(send[0, peer], BLOCKS - 1)]
        return carry

    repeat(DOMAINS // 8, hand_over)


def table_kernel(land, ghost, home, other, local_table, ghost_table):
    def by_pair(group, carry):
        for inner in range(8):
            entry = group * 8 + inner
            local_table[0, entry] = home[0, entry] + BLOCKS * other[0, entry]
        return carry

    lax.fori_loop(0, LOCAL // 8, by_pair, 0)

    def by_peer(group, carry):
        for inner in range(8):
            entry = LOCAL + group * 8 + inner
            peer = other[0, entry] - BLOCKS
            ghost_table[0, peer] = home[0, entry] + BLOCKS * (ghost[0, peer] + BLOCKS * land[0, peer])
        return carry

    lax.fori_loop(0, DOMAINS // 8, by_peer, 0)


def pair_of(table, entry):
    packed = table[0, entry]
    return packed & (BLOCKS - 1), (packed >> 6) & (BLOCKS - 1)


def place_kernel(table, states, arrived, placed, outgoing):
    def keep(group, carry):
        placed[pl.ds(group * 8, 8)] = states[pl.ds(group * 8, 8)]
        return carry

    repeat(BLOCKS // 8, keep)

    def receive(group, carry):
        for inner in range(8):
            peer = group * 8 + inner
            placed[table[0, peer] >> 12] = arrived[peer]
        return carry

    repeat(DOMAINS // 8, receive)

    def send(group, carry):
        for inner in range(8):
            peer = group * 8 + inner
            mate, sent = pair_of(table, peer)
            for which, slot in enumerate((sent, mate)):
                for column, row in enumerate((0, 1, 2, 6, 7)):
                    outgoing[peer, which : which + 1, column * BLOCK : (column + 1) * BLOCK] = (
                        placed[slot, row : row + 1, :]
                    )
        return carry

    repeat(DOMAINS // 8, send)


def local_kernel(table, placed, sums, targets, columns_of, weights, spread):
    def prepare(group):
        stacked = []
        for inner in range(4):
            block = group * 4 + inner
            state = placed[block]
            parts = exponent_parts(state[0:3])
            targets[block] = target_rows(parts)
            weights[block] = weight_rows(state[0:3], state[7:8])
            stacked.append(source_rows(parts, state[6:7]))
            sums[block] = jnp.zeros((16, BLOCK), f32)
        columns = jnp.concatenate(stacked, 0).T
        empty = jnp.zeros((BLOCK, BLOCK - 32), bf16)
        for inner in range(4):
            block = group * 4 + inner
            chosen = columns[:, inner * 32 : (inner + 1) * 32]
            columns_of[block] = jnp.concatenate([chosen.astype(bf16), empty], 1)
            spread[block] = jnp.broadcast_to(chosen[:, 24:25], (BLOCK, BLOCK))

    def prepare_some(chunk, carry):
        for inner in range(8):
            prepare(chunk * 8 + inner)
        return carry

    lax.fori_loop(0, BLOCKS // 32, prepare_some, 0)

    def pairs(group, carry):
        for inner in range(local_unroll):
            entry = group * local_unroll + inner
            one, two = pair_of(table, entry)
            result = coupled_sums(
                jnp.concatenate([columns_of[two], columns_of[one]], 1),
                (spread[two], spread[one]),
                (weights[two], weights[one]),
                (targets[one], targets[two]),
                (placed[one, 6:7, :], placed[two, 6:7, :]),
            )
            sums[one] += result[:16, :BLOCK]
            sums[two] += result[16:, BLOCK:]
        return carry

    repeat(LOCAL // local_unroll, pairs)


def ghost_pairs(table, placed, targets, sums, total, coords_of, params_of):
    def start(group, carry):
        total[pl.ds(group * 8, 8)] = sums[pl.ds(group * 8, 8)]
        return carry

    repeat(BLOCKS // 8, start)

    def pairs(group, carry):
        for half in range(ghost_unroll // 2):
            stacked = []
            weights = []
            for inner in range(2):
                peer = group * ghost_unroll + half * 2 + inner
                for which in range(2):
                    coords = coords_of(peer, which)
                    charge, weight = params_of(peer, which)
                    stacked.append(source_rows(exponent_parts(coords), charge))
                    weights.append(weight_rows(coords, weight))
            columns = jnp.concatenate(stacked, 0).T
            narrow = columns.astype(bf16)
            for inner in range(2):
                peer = group * ghost_unroll + half * 2 + inner
                one, two = pair_of(table, peer)
                lane = inner * 64
                result = coupled_sums(
                    narrow[:, lane : lane + 64],
                    (
                        jnp.broadcast_to(columns[:, lane + 24 : lane + 25], (BLOCK, BLOCK)),
                        jnp.broadcast_to(columns[:, lane + 56 : lane + 57], (BLOCK, BLOCK)),
                    ),
                    (weights[inner * 2], weights[inner * 2 + 1]),
                    (targets[one], targets[two]),
                    (placed[one, 6:7, :], placed[two, 6:7, :]),
                )
                total[one] += result[:16, :BLOCK]
                total[two] += result[16:, BLOCK:]
        return carry

    repeat(DOMAINS // ghost_unroll, pairs)


def moved(state, total):
    folded = total[0:4] + total[4:8] + total[8:12]
    force = (coupling_scale * state[7:8]) * (state[0:3] * folded[3:4] - folded[0:3])
    speed = state[3:6] + time_step * force
    return state[0:3] + time_step * speed, speed, force


def middle_kernel(table, placed, sums, targets, received, updated, outgoing, total):
    def row(peer, which, column):
        return received[peer, which : which + 1, column * BLOCK : (column + 1) * BLOCK]

    ghost_pairs(
        table,
        placed,
        targets,
        sums,
        total,
        lambda peer, which: jnp.concatenate([row(peer, which, c) for c in range(3)], 0),
        lambda peer, which: (row(peer, which, 3), row(peer, which, 4)),
    )

    def step(group, carry):
        for inner in range(8):
            block = group * 8 + inner
            state = placed[block]
            coords, speed, _ = moved(state, total[block])
            updated[block] = jnp.concatenate([coords, speed, state[6:8]], 0)
        return carry

    repeat(BLOCKS // 8, step)

    def send(group, carry):
        for inner in range(8):
            peer = group * 8 + inner
            mate, sent = pair_of(table, peer)
            for which, slot in enumerate((sent, mate)):
                for column in range(3):
                    outgoing[peer, which : which + 1, column * BLOCK : (column + 1) * BLOCK] = (
                        updated[slot, column : column + 1, :]
                    )
        return carry

    repeat(DOMAINS // 8, send)


def last_kernel(
    table,
    placed,
    sums,
    targets,
    received,
    earlier,
    coords_out,
    speeds_out,
    forces_out,
    total,
):
    def row(ref, peer, which, column):
        return ref[peer, which : which + 1, column * BLOCK : (column + 1) * BLOCK]

    ghost_pairs(
        table,
        placed,
        targets,
        sums,
        total,
        lambda peer, which: jnp.concatenate([row(received, peer, which, c) for c in range(3)], 0),
        lambda peer, which: (row(earlier, peer, which, 3), row(earlier, peer, which, 4)),
    )

    def step(group, carry):
        for inner in range(8):
            block = group * 8 + inner
            coords, speed, force = moved(placed[block], total[block])
            lanes = pl.ds(block * BLOCK, BLOCK)
            coords_out[:, lanes] = coords
            speeds_out[:, lanes] = speed
            forces_out[:, lanes] = force
        return carry

    repeat(BLOCKS // 8, step)


def grant(mebibytes):
    return pltpu.CompilerParams(vmem_limit_bytes=mebibytes << 20)


def shape(*dims, dtype=f32):
    return jax.ShapeDtypeStruct(dims, dtype)


def in_hbm(values):
    return pltpu.with_memory_space_constraint(values, pltpu.HBM)


def pack(scale, send, positions, velocities, charges, solute):
    return pl.pallas_call(
        pack_kernel,
        compiler_params=grant(4),
        in_specs=[smem, smem, vmem, vmem, vmem, vmem],
        out_specs=(vmem, vmem),
        out_shape=(shape(BLOCKS, 8, BLOCK), shape(DOMAINS, 8, BLOCK)),
    )(scale, *(in_hbm(x) for x in (send, positions, velocities, charges, solute)))


def tables(land, ghost, home, other):
    return pl.pallas_call(
        table_kernel,
        compiler_params=grant(1),
        in_specs=[smem, smem, smem, smem],
        out_specs=(smem, smem),
        out_shape=(shape(1, LOCAL, dtype=jnp.int32), shape(1, DOMAINS, dtype=jnp.int32)),
        cost_estimate=pl.CostEstimate(
            flops=100_000_000, transcendentals=0, bytes_accessed=10_000
        ),
    )(land, ghost, home, other)


def place(table, states, arrived):
    return pl.pallas_call(
        place_kernel,
        compiler_params=grant(4),
        in_specs=[smem, vmem, vmem],
        out_specs=(vmem, vmem),
        out_shape=(shape(BLOCKS + 1, 8, BLOCK), shape(DOMAINS, 2, 5 * BLOCK)),
    )(table, states, arrived)


def local_pairs(table, placed):
    return pl.pallas_call(
        local_kernel,
        compiler_params=grant(16),
        in_specs=[smem, vmem],
        out_specs=(vmem, vmem),
        out_shape=(shape(BLOCKS, 16, BLOCK), shape(BLOCKS, 32, BLOCK, dtype=bf16)),
        scratch_shapes=[
            pltpu.VMEM((BLOCKS, BLOCK, BLOCK), bf16),
            pltpu.VMEM((BLOCKS, 16, BLOCK), bf16),
            pltpu.VMEM((BLOCKS, BLOCK, BLOCK), f32),
        ],
        cost_estimate=pl.CostEstimate(
            flops=1_000_000_000, transcendentals=4_000_000, bytes_accessed=1_000_000
        ),
    )(table, placed)


def middle(table, placed, sums, targets, received):
    return pl.pallas_call(
        middle_kernel,
        compiler_params=grant(8),
        in_specs=[smem, vmem, vmem, vmem, vmem],
        out_specs=(vmem, vmem),
        out_shape=(shape(BLOCKS + 1, 8, BLOCK), shape(DOMAINS, 2, 3 * BLOCK)),
        scratch_shapes=[
            pltpu.VMEM((BLOCKS, 16, BLOCK), f32),
        ],
    )(table, placed, sums, targets, received)


def last(table, placed, sums, targets, received, earlier):
    flat = shape(3, BLOCKS * BLOCK)
    return pl.pallas_call(
        last_kernel,
        compiler_params=grant(8),
        in_specs=[smem, vmem, vmem, vmem, vmem, vmem],
        out_specs=(vmem, vmem, vmem),
        out_shape=(flat, flat, flat),
        scratch_shapes=[
            pltpu.VMEM((BLOCKS, 16, BLOCK), f32),
        ],
    )(table, placed, sums, targets, received, earlier)


def exchange(values):
    return lax.all_to_all(values, "dom", split_axis=0, concat_axis=0, tiled=True)


def on_device(
    positions,
    velocities,
    charges,
    solute,
    rest_scale,
    send_slot,
    land_slot,
    ghost_slot,
    pair_home,
    pair_other,
):
    states, outbound = pack(
        rest_scale,
        send_slot,
        positions,
        velocities,
        charges.reshape(BLOCKS, BLOCK),
        solute.reshape(BLOCKS, BLOCK),
    )
    arrived = exchange(outbound)
    local_table, ghost_table = tables(land_slot, ghost_slot, pair_home, pair_other)
    placed, outgoing = place(ghost_table, states, arrived)
    ghosts = exchange(outgoing)
    sums, targets = local_pairs(local_table, placed)
    placed, outgoing = middle(ghost_table, placed, sums, targets, ghosts)
    moved_ghosts = exchange(outgoing)
    sums, targets = local_pairs(local_table, placed)
    return last(ghost_table, placed, sums, targets, moved_ghosts, ghosts)


def solution(mesh):
    in_specs = (
        P(None, ("rep", "dom")),
        P(None, ("rep", "dom")),
        P(("rep", "dom")),
        P(("rep", "dom")),
        P("rep"),
        P(("rep", "dom"), None),
        P(("rep", "dom"), None),
        P(("rep", "dom"), None),
        P(("rep", "dom"), None),
        P(("rep", "dom"), None),
    )
    out_specs = (P(None, ("rep", "dom")), P(None, ("rep", "dom")), P(None, ("rep", "dom")))
    return jax.shard_map(
        on_device, mesh=mesh, in_specs=in_specs, out_specs=out_specs, check_vma=False
    )
```

```python
import math

import jax
import jax.numpy as jnp
from jax import lax
from jax.experimental import pallas as pl
from jax.experimental.pallas import tpu as pltpu
from jax.sharding import PartitionSpec as P

BLOCK = 128
BLOCKS = 64
DOMAINS = 64
LOCAL = 128

coupling_scale = 0.2
time_step = 0.05
root_log2e = math.sqrt(math.log2(math.e))
local_unroll = 128
ghost_unroll = 64
f32 = jnp.float32
bf16 = jnp.bfloat16

vmem = pl.BlockSpec(memory_space=pltpu.VMEM)
smem = pl.BlockSpec(memory_space=pltpu.SMEM)


def repeat(count, body):
    for index in range(count):
        body(index, 0)


def rounded(values):
    return values.astype(bf16).astype(f32)


def split3(values):
    first = rounded(values)
    rest = values - first
    second = rounded(rest)
    return first, second, rounded(rest - second)


def exponent_parts(coords):
    scaled = coords * root_log2e
    half = 0.5 * jnp.sum(scaled * scaled, 0, keepdims=True)
    return split3(jnp.concatenate([scaled, half, scaled, half], 0))


def row_masks():
    row = lax.broadcasted_iota(jnp.int32, (8, BLOCK), 0)
    return row == 3, row == 7, row < 4


def source_rows(parts, charge):
    p0, p1, p2 = parts
    third, last, low = row_masks()
    s0 = jnp.where(third, -p0, jnp.where(last, -p1, p0))
    s1 = jnp.where(third, -p2, jnp.where(last, 1.0, p1))
    s2 = jnp.where(third | last, 1.0, jnp.where(low, p0, p2))
    return jnp.concatenate([s0, s1, s2, jnp.broadcast_to(charge, (8, BLOCK))], 0)


def target_rows(parts):
    p0, p1, p2 = parts
    third, last, low = row_masks()
    t0 = jnp.where(third | last, 1.0, jnp.where(low, p0, p1))
    t1 = jnp.where(third, 1.0, jnp.where(last, -p0, jnp.where(low, p0, p1)))
    t2 = jnp.where(third, -p1, jnp.where(last, -p2, jnp.where(low, p2, p0)))
    return jnp.concatenate([t0, t1, t2, jnp.zeros((8, BLOCK), f32)], 0).astype(bf16)


def weight_rows(coords, weight):
    low = row_masks()[2]
    ones = jnp.ones((1, BLOCK), f32)
    w0, w1, w2 = split3(jnp.concatenate([coords, ones, coords, ones], 0) * weight)
    return jnp.concatenate([jnp.where(low, w0, w1), jnp.where(low, w2, 0.0)], 0).astype(bf16)


def paired_targets(parts):
    p0, p1, p2 = parts
    third, last, low = row_masks()
    fourth = third | last
    plain = jnp.where(fourth, 1.0, p0)
    steps = [
        plain,
        jnp.where(fourth, 1.0, p1),
        plain,
        jnp.where(fourth, -p0, p1),
        jnp.where(fourth, -p1, p2),
        jnp.where(fourth, -p2, p0),
    ]
    rest = [jnp.zeros((16, BLOCK), f32)]
    upper = jnp.concatenate([jnp.where(low, step, 0.0) for step in steps] + rest, 0)
    lower = jnp.concatenate([jnp.where(low, 0.0, step) for step in steps] + rest, 0)
    return upper.astype(bf16), lower.astype(bf16)


def paired_sources(coords, charges):
    third, last, low = row_masks()
    fourth = third | last
    rows = []
    for values in coords:
        scaled = values * root_log2e
        rows += [scaled, 0.5 * jnp.sum(scaled * scaled, 0, keepdims=True)]
    p0, p1, p2 = split3(jnp.concatenate(rows, 0))
    return [
        jnp.where(fourth, -p0, p0),
        jnp.where(fourth, -p1, p0),
        jnp.where(fourth, -p2, p1),
        jnp.where(fourth, 1.0, p1),
        jnp.where(fourth, 1.0, p0),
        jnp.where(fourth, 1.0, p2),
        jnp.where(low, charges[0], charges[1]),
        jnp.zeros((8, BLOCK), f32),
    ]


def paired_weights(coords, weights):
    low = row_masks()[2]
    ones = jnp.ones((1, BLOCK), f32)
    rows = jnp.concatenate([coords[0], ones, coords[1], ones], 0)
    parts = split3(rows * jnp.where(low, weights[0], weights[1]))
    return jnp.concatenate([*parts, jnp.zeros((8, BLOCK), f32)], 0).astype(bf16)


def local_right(targets):
    empty = jnp.zeros((32, BLOCK), bf16)
    gap = jnp.zeros((BLOCK - 32, 2 * BLOCK), bf16)
    return jnp.concatenate(
        [
            jnp.concatenate([targets[0], empty], 1),
            gap,
            jnp.concatenate([empty, targets[1]], 1),
            gap,
        ],
        0,
    )


def coupled_sums(sources, charges, left, right, target_charges):
    exponent = jnp.dot(sources, right, preferred_element_type=f32)
    tiles = []
    for which in range(2):
        decay = jnp.exp2(exponent[:, which * BLOCK : (which + 1) * BLOCK])
        tiles.append(decay * (charges[which] * target_charges[which] + decay))
    coupling = jnp.concatenate(tiles, 1)
    high = coupling.astype(bf16)
    low = (coupling - high.astype(f32)).astype(bf16)
    stacked = jnp.concatenate([high, low], 0)
    left = jnp.concatenate([left, left], 1)
    return jnp.dot(left, stacked, preferred_element_type=f32)


def pack_kernel(scale, send, positions, velocities, charges, solute, states, outbound):
    root = jnp.sqrt(jnp.full((8, BLOCK), scale[0], f32))

    def gather(group, carry):
        first = group * 8
        charge_rows = charges[pl.ds(first, 8), :]
        weight = jnp.where(solute[pl.ds(first, 8), :] == 1, root, 1.0)
        for inner in range(8):
            lanes = pl.ds((group * 8 + inner) * BLOCK, BLOCK)
            states[group * 8 + inner] = jnp.concatenate(
                [
                    positions[:, lanes],
                    velocities[:, lanes],
                    charge_rows[inner : inner + 1],
                    weight[inner : inner + 1],
                ],
                0,
            )
        return carry

    repeat(BLOCKS // 8, gather)

    def hand_over(group, carry):
        for inner in range(8):
            peer = group * 8 + inner
            outbound[peer] = states[jnp.minimum(send[0, peer], BLOCKS - 1)]
        return carry

    repeat(DOMAINS // 8, hand_over)


def table_kernel(land, ghost, home, other, local_table, ghost_table):
    def by_pair(group, carry):
        for inner in range(8):
            entry = group * 8 + inner
            local_table[0, entry] = home[0, entry] + BLOCKS * other[0, entry]
        return carry

    lax.fori_loop(0, LOCAL // 8, by_pair, 0)

    def by_peer(group, carry):
        for inner in range(8):
            entry = LOCAL + group * 8 + inner
            peer = other[0, entry] - BLOCKS
            ghost_table[0, peer] = home[0, entry] + BLOCKS * (ghost[0, peer] + BLOCKS * land[0, peer])
        return carry

    lax.fori_loop(0, DOMAINS // 8, by_peer, 0)


def pair_of(table, entry):
    packed = table[0, entry]
    return packed & (BLOCKS - 1), (packed >> 6) & (BLOCKS - 1)


def place_kernel(table, states, arrived, placed, outgoing):
    def keep(group, carry):
        placed[pl.ds(group * 8, 8)] = states[pl.ds(group * 8, 8)]
        return carry

    repeat(BLOCKS // 8, keep)

    def receive(group, carry):
        for inner in range(8):
            peer = group * 8 + inner
            placed[table[0, peer] >> 12] = arrived[peer]
        return carry

    repeat(DOMAINS // 8, receive)

    def send(group, carry):
        for inner in range(8):
            peer = group * 8 + inner
            mate, sent = pair_of(table, peer)
            for which, slot in enumerate((sent, mate)):
                for column, row in enumerate((0, 1, 2, 6, 7)):
                    outgoing[peer, which : which + 1, column * BLOCK : (column + 1) * BLOCK] = (
                        placed[slot, row : row + 1, :]
                    )
        return carry

    repeat(DOMAINS // 8, send)


def local_kernel(table, placed, sums, paired, targets, columns_of, weights, spread):
    def prepare(group):
        stacked = []
        for inner in range(4):
            block = group * 4 + inner
            state = placed[block]
            parts = exponent_parts(state[0:3])
            targets[block] = target_rows(parts)
            paired[block, 0], paired[block, 1] = paired_targets(parts)
            weights[block] = weight_rows(state[0:3], state[7:8])
            stacked.append(source_rows(parts, state[6:7]))
            sums[block] = jnp.zeros((16, BLOCK), f32)
        columns = jnp.concatenate(stacked, 0).T
        empty = jnp.zeros((BLOCK, BLOCK - 32), bf16)
        for inner in range(4):
            block = group * 4 + inner
            chosen = columns[:, inner * 32 : (inner + 1) * 32]
            columns_of[block] = jnp.concatenate([chosen.astype(bf16), empty], 1)
            spread[block] = jnp.broadcast_to(chosen[:, 24:25], (BLOCK, BLOCK))

    def prepare_some(chunk, carry):
        for inner in range(8):
            prepare(chunk * 8 + inner)
        return carry

    lax.fori_loop(0, BLOCKS // 32, prepare_some, 0)

    def pairs(group, carry):
        for inner in range(local_unroll):
            entry = group * local_unroll + inner
            one, two = pair_of(table, entry)
            result = coupled_sums(
                jnp.concatenate([columns_of[two], columns_of[one]], 1),
                (spread[two], spread[one]),
                jnp.concatenate([weights[two], weights[one]], 0),
                local_right((targets[one], targets[two])),
                (placed[one, 6:7, :], placed[two, 6:7, :]),
            )
            sums[one] += result[:16, :BLOCK]
            sums[two] += result[16:, BLOCK:]
        return carry

    repeat(LOCAL // local_unroll, pairs)


def ghost_pairs(table, placed, targets, sums, total, coords_of, params_of):
    def start(group, carry):
        total[pl.ds(group * 8, 8)] = sums[pl.ds(group * 8, 8)]
        return carry

    repeat(BLOCKS // 8, start)

    def pairs(group, carry):
        for half in range(ghost_unroll // 2):
            stacked = []
            lefts = []
            for inner in range(2):
                peer = group * ghost_unroll + half * 2 + inner
                coords = [coords_of(peer, which) for which in range(2)]
                params = [params_of(peer, which) for which in range(2)]
                stacked += paired_sources(coords, [param[0] for param in params])
                lefts.append(paired_weights(coords, [param[1] for param in params]))
            columns = jnp.concatenate(stacked, 0).T
            narrow = columns.astype(bf16)
            for inner in range(2):
                peer = group * ghost_unroll + half * 2 + inner
                one, two = pair_of(table, peer)
                lane = inner * 64
                result = coupled_sums(
                    narrow[:, lane : lane + 64],
                    (
                        jnp.broadcast_to(columns[:, lane + 48 : lane + 49], (BLOCK, BLOCK)),
                        jnp.broadcast_to(columns[:, lane + 52 : lane + 53], (BLOCK, BLOCK)),
                    ),
                    lefts[inner],
                    jnp.concatenate([targets[one, 0], targets[two, 1]], 1),
                    (placed[one, 6:7, :], placed[two, 6:7, :]),
                )
                folded = result[0:8] + result[8:16] + result[16:24]
                upper = row_masks()[2]
                total[one, 0:8] += jnp.where(upper, folded[:, :BLOCK], 0.0)
                total[two, 0:8] += jnp.where(upper, 0.0, folded[:, BLOCK:])
        return carry

    repeat(DOMAINS // ghost_unroll, pairs)


def moved(state, total):
    folded = total[0:4] + total[4:8] + total[8:12]
    force = (coupling_scale * state[7:8]) * (state[0:3] * folded[3:4] - folded[0:3])
    speed = state[3:6] + time_step * force
    return state[0:3] + time_step * speed, speed, force


def middle_kernel(table, placed, sums, targets, received, updated, outgoing, total):
    def row(peer, which, column):
        return received[peer, which : which + 1, column * BLOCK : (column + 1) * BLOCK]

    ghost_pairs(
        table,
        placed,
        targets,
        sums,
        total,
        lambda peer, which: jnp.concatenate([row(peer, which, c) for c in range(3)], 0),
        lambda peer, which: (row(peer, which, 3), row(peer, which, 4)),
    )

    def step(group, carry):
        for inner in range(8):
            block = group * 8 + inner
            state = placed[block]
            coords, speed, _ = moved(state, total[block])
            updated[block] = jnp.concatenate([coords, speed, state[6:8]], 0)
        return carry

    repeat(BLOCKS // 8, step)

    def send(group, carry):
        for inner in range(8):
            peer = group * 8 + inner
            mate, sent = pair_of(table, peer)
            for which, slot in enumerate((sent, mate)):
                for column in range(3):
                    outgoing[peer, which : which + 1, column * BLOCK : (column + 1) * BLOCK] = (
                        updated[slot, column : column + 1, :]
                    )
        return carry

    repeat(DOMAINS // 8, send)


def last_kernel(
    table,
    placed,
    sums,
    targets,
    received,
    earlier,
    coords_out,
    speeds_out,
    forces_out,
    total,
):
    def row(ref, peer, which, column):
        return ref[peer, which : which + 1, column * BLOCK : (column + 1) * BLOCK]

    ghost_pairs(
        table,
        placed,
        targets,
        sums,
        total,
        lambda peer, which: jnp.concatenate([row(received, peer, which, c) for c in range(3)], 0),
        lambda peer, which: (row(earlier, peer, which, 3), row(earlier, peer, which, 4)),
    )

    def step(group, carry):
        for inner in range(8):
            block = group * 8 + inner
            coords, speed, force = moved(placed[block], total[block])
            lanes = pl.ds(block * BLOCK, BLOCK)
            coords_out[:, lanes] = coords
            speeds_out[:, lanes] = speed
            forces_out[:, lanes] = force
        return carry

    repeat(BLOCKS // 8, step)


def grant(mebibytes):
    return pltpu.CompilerParams(vmem_limit_bytes=mebibytes << 20)


def shape(*dims, dtype=f32):
    return jax.ShapeDtypeStruct(dims, dtype)


def in_hbm(values):
    return pltpu.with_memory_space_constraint(values, pltpu.HBM)


def pack(scale, send, positions, velocities, charges, solute):
    return pl.pallas_call(
        pack_kernel,
        compiler_params=grant(4),
        in_specs=[smem, smem, vmem, vmem, vmem, vmem],
        out_specs=(vmem, vmem),
        out_shape=(shape(BLOCKS, 8, BLOCK), shape(DOMAINS, 8, BLOCK)),
    )(scale, *(in_hbm(x) for x in (send, positions, velocities, charges, solute)))


def tables(land, ghost, home, other):
    return pl.pallas_call(
        table_kernel,
        compiler_params=grant(1),
        in_specs=[smem, smem, smem, smem],
        out_specs=(smem, smem),
        out_shape=(shape(1, LOCAL, dtype=jnp.int32), shape(1, DOMAINS, dtype=jnp.int32)),
        cost_estimate=pl.CostEstimate(
            flops=100_000_000, transcendentals=0, bytes_accessed=10_000
        ),
    )(land, ghost, home, other)


def place(table, states, arrived):
    return pl.pallas_call(
        place_kernel,
        compiler_params=grant(4),
        in_specs=[smem, vmem, vmem],
        out_specs=(vmem, vmem),
        out_shape=(shape(BLOCKS + 1, 8, BLOCK), shape(DOMAINS, 2, 5 * BLOCK)),
    )(table, states, arrived)


def local_pairs(table, placed):
    return pl.pallas_call(
        local_kernel,
        compiler_params=grant(16),
        in_specs=[smem, vmem],
        out_specs=(vmem, vmem),
        out_shape=(shape(BLOCKS, 16, BLOCK), shape(BLOCKS, 2, 64, BLOCK, dtype=bf16)),
        scratch_shapes=[
            pltpu.VMEM((BLOCKS, 32, BLOCK), bf16),
            pltpu.VMEM((BLOCKS, BLOCK, BLOCK), bf16),
            pltpu.VMEM((BLOCKS, 16, BLOCK), bf16),
            pltpu.VMEM((BLOCKS, BLOCK, BLOCK), f32),
        ],
        cost_estimate=pl.CostEstimate(
            flops=1_000_000_000, transcendentals=4_000_000, bytes_accessed=1_000_000
        ),
    )(table, placed)


def middle(table, placed, sums, targets, received):
    return pl.pallas_call(
        middle_kernel,
        compiler_params=grant(8),
        in_specs=[smem, vmem, vmem, vmem, vmem],
        out_specs=(vmem, vmem),
        out_shape=(shape(BLOCKS + 1, 8, BLOCK), shape(DOMAINS, 2, 3 * BLOCK)),
        scratch_shapes=[
            pltpu.VMEM((BLOCKS, 16, BLOCK), f32),
        ],
    )(table, pltpu.with_memory_space_constraint(placed, pltpu.VMEM), sums, targets, received)


def last(table, placed, sums, targets, received, earlier):
    flat = shape(3, BLOCKS * BLOCK)
    return pl.pallas_call(
        last_kernel,
        compiler_params=grant(8),
        in_specs=[smem, vmem, vmem, vmem, vmem, vmem],
        out_specs=(vmem, vmem, vmem),
        out_shape=(flat, flat, flat),
        scratch_shapes=[
            pltpu.VMEM((BLOCKS, 16, BLOCK), f32),
        ],
    )(table, placed, sums, targets, received, earlier)


def exchange(values):
    return lax.all_to_all(values, "dom", split_axis=0, concat_axis=0, tiled=True)


def on_device(
    positions,
    velocities,
    charges,
    solute,
    rest_scale,
    send_slot,
    land_slot,
    ghost_slot,
    pair_home,
    pair_other,
):
    states, outbound = pack(
        rest_scale,
        send_slot,
        positions,
        velocities,
        charges.reshape(BLOCKS, BLOCK),
        solute.reshape(BLOCKS, BLOCK),
    )
    arrived = exchange(outbound)
    local_table, ghost_table = tables(land_slot, ghost_slot, pair_home, pair_other)
    placed, outgoing = place(ghost_table, states, arrived)
    ghosts = exchange(outgoing)
    sums, targets = local_pairs(local_table, placed)
    placed, outgoing = middle(ghost_table, placed, sums, targets, ghosts)
    moved_ghosts = exchange(outgoing)
    sums, targets = local_pairs(local_table, placed)
    return last(ghost_table, placed, sums, targets, moved_ghosts, ghosts)


def solution(mesh):
    in_specs = (
        P(None, ("rep", "dom")),
        P(None, ("rep", "dom")),
        P(("rep", "dom")),
        P(("rep", "dom")),
        P("rep"),
        P(("rep", "dom"), None),
        P(("rep", "dom"), None),
        P(("rep", "dom"), None),
        P(("rep", "dom"), None),
        P(("rep", "dom"), None),
    )
    out_specs = (P(None, ("rep", "dom")), P(None, ("rep", "dom")), P(None, ("rep", "dom")))
    return jax.shard_map(
        on_device, mesh=mesh, in_specs=in_specs, out_specs=out_specs, check_vma=False
    )
```
